128 devices in a mesh: dp: 32 (over z, y, x_hi), section: 2 (over core), tensor: 2 (over x_lo).
Axes of the slice: x: 4 (x_hi: 2, x_lo: 2; x = x_hi * 2 + x_lo), y: 4, z: 4, core: 2. Of those that a mesh axis runs over, the one named last changes fastest.
Arguments:
- tokens: bfloat16 [512, 32, 1024], P('dp'), may hold values from -6 to 6
- counts: int32 [512], replicated, may hold values from 8 to 32, as said below
- assign: int32 [512], replicated, may hold values from 0 to 511, as said below
- qkv_weight: bfloat16 [2, 1024, 3, 1024], P('section', 'dp', None, 'tensor'), may hold values from -0.9375 to 0.9375
- out_weight: bfloat16 [2, 1024, 1024], P('section', 'dp'), may hold values from -0.1875 to 0.1875
- up_weight: bfloat16 [2, 1024, 4096], P('section', 'dp', 'tensor'), may hold values from -0.1875 to 0.1875
- up_bias: bfloat16 [2, 4096], P('section', 'tensor'), may hold values from -3 to 3
- down_weight: bfloat16 [2, 4096, 1024], P('section', 'tensor', 'dp'), may hold values from -0.09375 to 0.09375
- attn_gain: bfloat16 [2, 1024], P('section'), may hold values from 0.25 to 1.75
- mlp_gain: bfloat16 [2, 1024], P('section'), may hold values from 0.25 to 1.75
- final_gain: bfloat16 [1024], replicated, may hold values from 0.25 to 1.75
Outputs:
- encoded: bfloat16 [512, 32, 1024], P('dp', 'section', 'tensor')
The draws below stay inside these ranges and needn't reach their ends.
Inputs may be any that keep to these rules, and one draw needn't show every extreme that they name: `counts`: every count is at least 8, and in every draw some image has all 32 slots live. assign is a permutation of the images. Slot j belongs to data group j // 16, so every data group receives 16 images; within one data group's slots the images stand in increasing order. Images of data group g are tokens rows g * 16 to (g + 1) * 16 - 1. No data group hands more than 1 images to one data group (itself included), and in every draw some pair of data groups exchanges exactly 1. Every data group receives some image from the data group half the axis away.
All inputs are finite; a program needn't handle non-finite values.
Results may differ from the reference program's by a relative error of at most 0.024.
The reference program's roundings to bfloat16 on the way count: a program that leaves them out, or rounds other values in their place, can miss the bound.
Values may be sent and summed in bfloat16 or wider, within the bound.
No kernel may reach another device: no remote copies, remote signals or barrier semaphores. Data moves between devices by JAX's collectives and lax.ppermute only.
A program may use at most 128 MiB of HBM per device.

```python
import jax
import jax.numpy as jnp
from jax import lax

D = 1024
FF = 4096
BLOCK = 32
IMG_DEV = 16
HEAD_DIM = 64
LAYERS = 2
IMAGES = 512
CAP = 1
N_TENSOR = 2


def draw_counts(key, part):
    first_key, second_key = jax.random.split(jax.random.fold_in(key, 7))
    values = jax.random.randint(first_key, (IMAGES,), BLOCK // 4, BLOCK + 1)
    chosen_image = jax.random.randint(second_key, (), 0, IMAGES)
    return jnp.where(jnp.arange(IMAGES) == chosen_image, BLOCK, values).astype(jnp.int32)


def draw_assign(key, part):
    groups = IMAGES // IMG_DEV
    base_key = jax.random.fold_in(key, 11)
    order_key, shuffle_key = jax.random.split(base_key, 2)
    offsets_pool = jnp.repeat(jnp.arange(groups, dtype=jnp.int32), CAP)
    favoured = groups // 2
    order_score = jax.random.permutation(order_key, groups * CAP).astype(jnp.int32)
    order_score = jnp.where(offsets_pool == favoured, order_score - groups * CAP, order_score)
    taken = offsets_pool[jnp.argsort(order_score)[:IMG_DEV]]
    offsets = jax.random.permutation(shuffle_key, taken)
    group_numbers = jnp.arange(groups, dtype=jnp.int32)
    local_order = jax.vmap(lambda number: jax.random.permutation(jax.random.fold_in(base_key, 100 + number), IMG_DEV))(group_numbers)
    target_group = (group_numbers[:, None] + offsets[None, :]) % groups
    image_index = group_numbers[:, None] * IMG_DEV + local_order
    destination = jnp.zeros((IMAGES,), jnp.int32).at[image_index.reshape(-1)].set(target_group.reshape(-1).astype(jnp.int32))
    return jnp.argsort(destination * IMAGES + jnp.arange(IMAGES, dtype=jnp.int32)).astype(jnp.int32)


def draw_qkv_weight(key, part):
    values = jnp.clip(jax.random.normal(jax.random.fold_in(key, 13), (LAYERS, D, 3, D), jnp.float32), -5.0, 5.0) * D ** (-0.5)
    return values.astype(jnp.bfloat16)


def steps_of(stream_key, dims, pieces, low, largest):
    gain, own = 1.0, jax.random.fold_in(stream_key, 6)
    for dim, parts in pieces:
        steps = jnp.exp(jax.random.uniform(jax.random.fold_in(own, dim), (parts,), jnp.float32, low / len(pieces), largest / len(pieces)))
        gain = gain * jnp.repeat(steps, dims[dim] // parts).reshape([-1 if axis == dim else 1 for axis in range(len(dims))])
    return gain


def bell_draw(key, extent, scale, limit, pieces=(), kind=jnp.bfloat16):
    level = steps_of(key, extent, pieces, -0.22, 0.18) if pieces else 1.0
    values = jax.random.normal(key, extent, jnp.float32) * scale * level
    return jnp.minimum(jnp.maximum(values, -limit), limit).astype(kind)


def setup_inputs(seed: int = 0) -> dict:
    streams_of = jax.random.split(jax.random.key(seed), 12)
    return {
        "tokens": bell_draw(streams_of[0], (IMAGES, BLOCK, D), 1.0, 6.0, ((0, 32),)),
        "counts": draw_counts(jax.random.fold_in(streams_of[11], 71), 0),
        "assign": draw_assign(jax.random.fold_in(streams_of[11], 71), 0),
        "qkv_weight": draw_qkv_weight(jax.random.fold_in(streams_of[11], 71), 0),
        "out_weight": bell_draw(streams_of[4], (LAYERS, D, D), D ** -0.5, 0.1875, ((0, 2), (1, 32))),
        "up_weight": bell_draw(streams_of[5], (LAYERS, D, FF), D ** -0.5, 0.1875, ((0, 2), (1, 32), (2, 2))),
        "up_bias": bell_draw(streams_of[6], (LAYERS, FF), 0.5, 3.0, ((0, 2), (1, 2))),
        "down_weight": bell_draw(streams_of[7], (LAYERS, FF, D), FF ** -0.5, 0.09375, ((0, 2), (1, 2), (2, 32))),
        "attn_gain": jnp.clip(1.0 + 0.15 * jax.random.normal(streams_of[8], (LAYERS, D), jnp.float32), 0.25, 1.75).astype(jnp.bfloat16),
        "mlp_gain": jnp.clip(1.0 + 0.15 * jax.random.normal(streams_of[9], (LAYERS, D), jnp.float32), 0.25, 1.75).astype(jnp.bfloat16),
        "final_gain": jnp.clip(1.0 + 0.15 * jax.random.normal(streams_of[10], (D,), jnp.float32), 0.25, 1.75).astype(jnp.bfloat16),
    }


epsilon = 1e-06

def layer_norm(values, gain_vector):
    average = lax.optimization_barrier(jnp.mean(values, axis=-1, keepdims=True))
    centred = values - average
    spread = lax.optimization_barrier(jnp.mean(centred * centred, axis=-1, keepdims=True))
    return centred * lax.rsqrt(spread + epsilon) * gain_vector.astype(jnp.float32)

def attend(normed, w_merged, live_count, head_dim):
    row_count = normed.shape[0]
    merged = jnp.dot(normed, w_merged.reshape(w_merged.shape[0], -1), preferred_element_type=jnp.float32)
    merged = merged.reshape(row_count, 3, -1, head_dim)
    scores = jnp.einsum('qhd,khd->hqk', merged[:, 0], merged[:, 1], precision=lax.Precision.HIGHEST) * head_dim ** (-0.5)
    visible = jnp.arange(row_count) < live_count
    scores = jnp.where(visible[None, None, :], scores, -1e+30)
    weights = jax.nn.softmax(scores, axis=-1)
    mixed = jnp.einsum('hqk,khd->qhd', weights, merged[:, 2], precision=lax.Precision.HIGHEST)
    return mixed.reshape(row_count, -1).astype(jnp.bfloat16)

def reference(tokens, counts, assign, qkv_weight, out_weight, up_weight, up_bias, down_weight, attn_gain, mlp_gain, final_gain):
    stream = tokens[assign]
    live_counts = counts[assign]
    images, block_rows, model_width = stream.shape
    quarter = FF // N_TENSOR

    def one_layer(stream, layer_weights):
        qkv_full, out_full, up_full, bias_row, down_full, gain_attn, gain_mlp = layer_weights
        normed = layer_norm(stream.astype(jnp.float32), gain_attn).astype(jnp.bfloat16)
        head_out = jax.vmap(lambda image_rows, live_count: attend(image_rows, qkv_full, live_count, HEAD_DIM))(normed, live_counts)
        flat = head_out.reshape(images * block_rows, model_width)
        middle = stream.reshape(-1, model_width).astype(jnp.float32) + jnp.dot(flat, out_full, preferred_element_type=jnp.float32)
        normed_mlp = layer_norm(middle, gain_mlp).astype(jnp.bfloat16)
        hidden = jax.nn.gelu(jnp.dot(normed_mlp, up_full, preferred_element_type=jnp.float32) + bias_row.astype(jnp.float32), approximate=False).astype(jnp.bfloat16)
        summed = jnp.zeros_like(middle)
        for shard_index in range(N_TENSOR):
            lower = shard_index * quarter
            partial_value = jnp.dot(hidden[:, lower:lower + quarter], down_full[lower:lower + quarter], preferred_element_type=jnp.float32)
            rounded = lax.optimization_barrier(partial_value.astype(jnp.bfloat16))
            summed = summed + rounded.astype(jnp.float32)
        updated = (middle + summed).astype(jnp.bfloat16)
        return (updated.reshape(images, block_rows, model_width), None)
    stream, _ = lax.scan(one_layer, stream, (qkv_weight, out_weight, up_weight, up_bias, down_weight, attn_gain, mlp_gain))
    visible = jnp.arange(block_rows)[None, :, None] < live_counts[:, None, None]
    normed_out = layer_norm(stream.astype(jnp.float32), final_gain)
    return jnp.where(visible, normed_out, 0.0).astype(jnp.bfloat16)
```

```python
import functools

import jax
import jax.numpy as jnp
from jax import lax
from jax.experimental import pallas as pl
from jax.experimental.pallas import tpu as pltpu
from jax.sharding import PartitionSpec as P

HEAD_DIM = 64
AXES = ("dp", "section", "tensor")
SIDE = 4
OFFSETS = (0, 3, 1, 2)
EPSILON = 1e-06
FAR = -1e30
BF16 = jnp.bfloat16
F32 = jnp.float32


def flat_id(z, y, xh, s, t):
    return (((z % SIDE) * SIDE + y % SIDE) * 2 + xh % 2) * 4 + (s % 2) * 2 + t % 2


def pairs_of(move):
    span = [
        (z, y, xh, s, t)
        for z in range(SIDE)
        for y in range(SIDE)
        for xh in range(2)
        for s in range(2)
        for t in range(2)
    ]
    return [(flat_id(*p), flat_id(*move(*p))) for p in span]


OVER_CORE = pairs_of(lambda z, y, xh, s, t: (z, y, xh, s + 1, t))
OVER_X = pairs_of(lambda z, y, xh, s, t: (z, y, xh + 1, s, t))
OVER_TENSOR = pairs_of(lambda z, y, xh, s, t: (z, y, xh, s, t + 1))


def first_ring(by):
    return pairs_of(
        lambda z, y, xh, s, t: (z, y + by, xh, s, t) if s == 0 else (z + by, y, xh, s, t)
    )


def second_ring(by):
    return pairs_of(
        lambda z, y, xh, s, t: (z + by, y, xh, s, t) if s == 0 else (z, y + by, xh, s, t)
    )


def sent(value, pairs):
    return lax.ppermute(value, AXES, pairs)


def layer_norm(values, gain_vector):
    average = jnp.mean(values, axis=-1, keepdims=True)
    centred = values - average
    spread = jnp.mean(centred * centred, axis=-1, keepdims=True)
    return centred * lax.rsqrt(spread + EPSILON) * gain_vector.astype(F32)


def load_weight(spots, own, other, first, second, sem, lower, width):
    at_core, at_z, at_y = spots[0], spots[1], spots[2]

    def start(sources, spread):
        into, at = (second, at_y) if spread else (first, at_z)
        for piece, offset in zip(sources, OFFSETS):
            spot = lax.rem(at + offset, SIDE)
            if spread:
                for row in range(SIDE):
                    pltpu.make_async_copy(
                        piece.at[pl.ds(row * 64, 64), pl.ds(lower, width)],
                        into.at[pl.ds(row * 256 + spot * 64, 64), :],
                        sem,
                    ).start()
            else:
                pltpu.make_async_copy(
                    piece.at[:, pl.ds(lower, width)], into.at[pl.ds(spot * 256, 256), :], sem
                ).start()

    @pl.when(at_core == 0)
    def _():
        start(own, False)
        start(other, True)

    @pl.when(at_core != 0)
    def _():
        start(other, False)
        start(own, True)


def wait_weight(first, second, sem):
    pltpu.make_async_copy(first, first, sem).wait()
    pltpu.make_async_copy(second, second, sem).wait()


def attention_body(fresh, *refs):
    spots, key_live = refs[0], refs[1]
    if fresh:
        stream_ref, gain = refs[2], refs[3]
        rest = refs[4:]
    else:
        middle, mine, theirs, gain = refs[2:6]
        rest = refs[6:]
    own, other = rest[:4], rest[4:8]
    rest = rest[8:]
    if fresh:
        head_out = rest[0]
        rest = rest[1:]
    else:
        head_out, stream_out = rest[:2]
        rest = rest[2:]
    first, second, normed, merged, sem = rest
    load_weight(spots, own, other, first, second, sem, 0, 768)
    if fresh:
        stream = stream_ref[...].astype(F32)
    else:
        summed = mine[...].astype(F32) + theirs[...].astype(F32)
        rounded = (middle[...] + summed).astype(BF16)
        stream_out[...] = rounded
        stream = rounded.astype(F32)
    normed[...] = layer_norm(stream, gain[...]).astype(BF16)
    wait_weight(first, second, sem)
    rows = lax.broadcasted_iota(jnp.int32, (256, 128), 0)
    cols = lax.broadcasted_iota(jnp.int32, (256, 128), 1)
    same = lax.rem(rows, 128) // 32 == cols // 32
    upper = rows >= 128
    chosen = upper == (cols >= 64)
    left = lax.broadcasted_iota(jnp.int32, (128, 128), 1) < 64
    for half, weight in enumerate((first, second)):
        merged[...] = jnp.dot(normed[...], weight[...], preferred_element_type=F32)
        for block in range(2):
            span = pl.ds(block * 128, 128)
            visible = same & (key_live[pl.ds(block, 1), :] > 0)
            for pair in range(2):
                query = merged[span, pl.ds(pair * 128, 128)] * HEAD_DIM ** (-0.5)
                key = merged[span, pl.ds(256 + pair * 128, 128)]
                value = merged[span, pl.ds(512 + pair * 128, 128)].astype(BF16)
                query = jnp.where(chosen, jnp.concatenate([query, query], 0), 0.0)
                query_high = query.astype(BF16)
                query_low = (query - query_high.astype(F32)).astype(BF16)
                key_high = key.astype(BF16)
                key_low = (key - key_high.astype(F32)).astype(BF16)
                over = (((1,), (1,)), ((), ()))
                scores = lax.dot_general(
                    jnp.concatenate([query_high, query_low], 1),
                    jnp.concatenate([key_high, key_high], 1),
                    over,
                    preferred_element_type=F32,
                ) + lax.dot_general(query_high, key_low, over, preferred_element_type=F32)
                scores = jnp.where(visible, scores, FAR)
                scores = jnp.exp(scores - jnp.max(scores, axis=-1, keepdims=True))
                total = jnp.sum(scores, axis=-1, keepdims=True)
                mixed = jnp.dot(scores.astype(BF16), value, preferred_element_type=F32) / total
                head_out[span, pl.ds(half * 256 + pair * 128, 128)] = jnp.where(
                    left, mixed[:128], mixed[128:]
                ).astype(BF16)


def mlp_body(*refs):
    spots, stream, mine, theirs, gain, bias = refs[:6]
    own_a, other_a, own_b, other_b = refs[6:10], refs[10:14], refs[14:18], refs[18:22]
    middle, partial = refs[22:24]
    out_first, out_second, up_first, up_second, down_first, down_second = refs[24:30]
    sem_out, sem_up, sem_down = refs[30:33]
    load_weight(spots, own_a, other_a, out_first, out_second, sem_out, 768, 512)
    load_weight(spots, own_b, other_b, up_first, up_second, sem_up, 0, 1024)
    load_weight(spots, own_b, other_b, down_first, down_second, sem_down, 1024, 1024)
    rank = spots[3]
    near, far = pl.ds(rank * 512, 512), pl.ds((1 - rank) * 512, 512)
    wait_weight(out_first, out_second, sem_out)
    for half, weight in enumerate((out_first, out_second)):
        span = pl.ds(half * 512, 512)
        middle[:, span] = (
            stream[:, span].astype(F32)
            + jnp.dot(mine[...], weight[near, :], preferred_element_type=F32)
            + jnp.dot(theirs[...], weight[far, :], preferred_element_type=F32)
        )
    normed = layer_norm(middle[...], gain[...]).astype(BF16)
    wait_weight(up_first, up_second, sem_up)
    hidden = []
    for half, weight in enumerate((up_first, up_second)):
        raised = jnp.dot(normed, weight[...], preferred_element_type=F32)
        raised = raised + bias[:, pl.ds(half * 1024, 1024)].astype(F32)
        hidden.append((raised * (0.5 + 0.5 * lax.erf(raised * 0.5**0.5))).astype(BF16))
    wait_weight(down_first, down_second, sem_down)
    over = (((1,), (1,)), ((), ()))
    partial[...] = (
        lax.dot_general(hidden[0], down_first[...], over, preferred_element_type=F32)
        + lax.dot_general(hidden[1], down_second[...], over, preferred_element_type=F32)
    ).astype(BF16)


def finish_body(spots, middle, mine, theirs, gain, row_live, kept, passed):
    summed = mine[...].astype(F32) + theirs[...].astype(F32)
    stream = (middle[...] + summed).astype(BF16).astype(F32)
    normed = jnp.where(row_live[...] > 0, layer_norm(stream, gain[...]), 0.0)
    normed = jnp.where(spots[3] == 0, normed[:, :512], normed[:, 512:])
    halves = normed.reshape(8, 2, 16, 512)
    upper, lower = halves[:, 0].reshape(128, 512), halves[:, 1].reshape(128, 512)
    kept[...] = jnp.where(spots[0] == 0, upper, lower).astype(BF16)
    passed[...] = jnp.where(spots[0] == 0, lower, upper).astype(BF16)


SMEM = pl.BlockSpec(memory_space=pltpu.SMEM)
VMEM = pl.BlockSpec(memory_space=pltpu.VMEM)
ANY = pl.BlockSpec(memory_space=pl.ANY)
PARAMS = pltpu.CompilerParams(vmem_limit_bytes=48 * 1024 * 1024)


def attention_call(spots, key_live, entry, gain, own, other):
    fresh = len(entry) == 1
    head = jax.ShapeDtypeStruct((256, 512), BF16)
    outs = head if fresh else (head, jax.ShapeDtypeStruct((256, 1024), BF16))
    return pl.pallas_call(
        functools.partial(attention_body, fresh),
        in_specs=[SMEM] + [VMEM] * (2 + len(entry)) + [ANY] * 8,
        out_specs=VMEM if fresh else (VMEM, VMEM),
        out_shape=outs,
        scratch_shapes=[
            pltpu.VMEM((1024, 768), BF16),
            pltpu.VMEM((1024, 768), BF16),
            pltpu.VMEM((256, 1024), BF16),
            pltpu.VMEM((256, 768), F32),
            pltpu.SemaphoreType.DMA,
        ],
        compiler_params=PARAMS,
        cost_estimate=pl.CostEstimate(
            flops=1_600_000_000, transcendentals=300_000, bytes_accessed=6_000_000
        ),
        name="attention",
    )(spots, key_live, *entry, gain, *own, *other)


def mlp_call(spots, stream, mine, theirs, gain, bias, own_a, other_a, own_b, other_b):
    return pl.pallas_call(
        mlp_body,
        in_specs=[SMEM] + [VMEM] * 5 + [ANY] * 16,
        out_specs=(VMEM, VMEM),
        out_shape=(
            jax.ShapeDtypeStruct((256, 1024), F32),
            jax.ShapeDtypeStruct((256, 1024), BF16),
        ),
        scratch_shapes=[
            pltpu.VMEM((1024, 512), BF16),
            pltpu.VMEM((1024, 512), BF16),
            pltpu.VMEM((1024, 1024), BF16),
            pltpu.VMEM((1024, 1024), BF16),
            pltpu.VMEM((1024, 1024), BF16),
            pltpu.VMEM((1024, 1024), BF16),
            pltpu.SemaphoreType.DMA,
            pltpu.SemaphoreType.DMA,
            pltpu.SemaphoreType.DMA,
        ],
        compiler_params=PARAMS,
        cost_estimate=pl.CostEstimate(
            flops=2_700_000_000, transcendentals=500_000, bytes_accessed=12_000_000
        ),
        name="mlp",
    )(spots, stream, mine, theirs, gain, bias, *own_a, *other_a, *own_b, *other_b)


def finish_call(spots, middle, mine, theirs, gain, row_live):
    half = jax.ShapeDtypeStruct((128, 512), BF16)
    return pl.pallas_call(
        finish_body,
        in_specs=[SMEM] + [VMEM] * 5,
        out_specs=(VMEM, VMEM),
        out_shape=(half, half),
        compiler_params=PARAMS,
        name="finish",
    )(spots, middle, mine, theirs, gain, row_live)


def placed(parts, at):
    rows, width = parts[0].shape
    whole = jnp.zeros((SIDE * rows, width), parts[0].dtype)
    for part, offset in zip(parts, OFFSETS):
        whole = lax.dynamic_update_slice(whole, part, (lax.rem(at + offset, SIDE) * rows, 0))
    return whole


def local(
    tokens,
    counts,
    assign,
    qkv_weight,
    out_weight,
    up_weight,
    up_bias,
    down_weight,
    attn_gain,
    mlp_gain,
    final_gain,
):
    dp, s, t = (lax.axis_index(name) for name in AXES)
    z, y, xh = dp // 8, (dp // 2) % SIDE, dp % 2
    spots = jnp.stack([s, z, y, t]).astype(jnp.int32)
    at_first = jnp.where(s == 0, y, z)

    colours = []
    turned = down_weight[0].T
    for c in range(2):
        colours.append(
            jnp.concatenate(
                [qkv_weight[0, :, k, c * 256 : c * 256 + 256] for k in range(3)]
                + [
                    out_weight[0, :, c * 512 : c * 512 + 512],
                    up_weight[0, :, c * 1024 : c * 1024 + 1024],
                    turned[:, c * 1024 : c * 1024 + 1024],
                ],
                axis=1,
            )
        )
    small = jnp.concatenate([up_bias[0], attn_gain[0], mlp_gain[0]]).reshape(32, 128)
    kept = jnp.where(s == 0, colours[0], colours[1])
    given = jnp.where(s == 0, colours[1], colours[0])
    got = sent(jnp.concatenate([given, small], axis=1), OVER_CORE)
    got, small_got = got[:, :3328], got[:, 3328:]
    layers = (jnp.where(s == 0, kept, got), jnp.where(s == 0, got, kept))
    smalls = (jnp.where(s == 0, small, small_got), jnp.where(s == 0, small_got, small))
    smalls = [v.reshape(1, 4096) for v in smalls]

    pieces = []
    for layer in range(2):
        with jax.named_scope(f"xhi{layer}"):
            partner = sent(layers[layer], OVER_X)
            pair = jnp.concatenate(
                [
                    jnp.where(xh == 0, layers[layer], partner),
                    jnp.where(xh == 0, partner, layers[layer]),
                ],
                axis=0,
            )
        with jax.named_scope(f"first{layer}"):
            parts = (pair,) + tuple(sent(pair, first_ring(by)) for by in (1, -1, 2))
            plane_a = placed([p[:, :1280] for p in parts], at_first)
            plane_b = placed([p[:, 1280:] for p in parts], at_first)
        for name, plane, by in (("a", plane_a, 1), ("b", plane_b, -1)):
            by = by if layer == 0 else -by
            with jax.named_scope(f"second{layer}{name}"):
                before = sent(plane, second_ring(1))
                after = sent(plane, second_ring(-1))
            with jax.named_scope(f"forward{layer}{name}"):
                across = sent(before if by == 1 else after, second_ring(by))
            own = (plane, before, after, across)
            with jax.named_scope(f"share{layer}{name}"):
                other = tuple(sent(v, OVER_CORE) for v in own)
            pieces.append((own, other))

    groups = 32
    table = assign.reshape(groups, 16)
    mine = lax.dynamic_slice_in_dim(assign, dp * 16, 16)
    lanes = jnp.arange(16, dtype=jnp.int32)
    selector = jnp.any(table[:, :, None] == (dp * 16 + lanes)[None, None, :], axis=1)
    quarter = 2 * t + s
    rows = lax.dynamic_slice_in_dim(tokens, quarter * 8, 8, 1)
    outgoing = jnp.einsum(
        "gl,lbd->gbd", selector.astype(BF16), rows, preferred_element_type=F32
    ).astype(BF16)
    received = lax.all_to_all(
        outgoing[:, None], "dp", split_axis=0, concat_axis=0, tiled=True
    )[:, 0]
    sources = (mine // 16).reshape(2, 8)
    numbers = jnp.arange(groups, dtype=jnp.int32)

    def picked(which):
        picker = (numbers[None, :] == which[:, None]).astype(BF16)
        return jnp.einsum(
            "js,sbd->jbd", picker, received, preferred_element_type=F32
        ).astype(BF16)

    stay = picked(jnp.where(s == 0, sources[0], sources[1]))
    leave = picked(jnp.where(s == 0, sources[1], sources[0]))
    came = sent(leave, OVER_CORE)
    half = jnp.concatenate(
        [jnp.where(s == 0, stay, came), jnp.where(s == 0, came, stay)], axis=1
    )
    far_half = sent(half, OVER_TENSOR)
    stream = jnp.concatenate(
        [jnp.where(t == 0, half, far_half), jnp.where(t == 0, far_half, half)], axis=1
    ).reshape(256, 1024)

    images = jnp.arange(counts.shape[0], dtype=jnp.int32)
    held = lax.dynamic_slice_in_dim(mine, s * 8, 8)
    live = jnp.sum(jnp.where(held[:, None] == images[None, :], counts[None, :], 0), axis=1)
    alive = (jnp.arange(32)[None, :] < live[:, None]).astype(F32)
    key_live = alive.reshape(2, 128)
    row_live = alive.reshape(256, 1)

    entry = (stream,)
    for layer in range(2):
        (own_a, other_a), (own_b, other_b) = pieces[2 * layer], pieces[2 * layer + 1]
        bias = smalls[layer][:, :2048]
        gain_attn = smalls[layer][:, 2048:3072]
        gain_mlp = smalls[layer][:, 3072:]
        made = attention_call(spots, key_live, entry, gain_attn, own_a, other_a)
        head, stream = (made, stream) if layer == 0 else made
        with jax.named_scope(f"heads{layer}"):
            theirs = sent(head, OVER_TENSOR)
        middle, partial = mlp_call(
            spots, stream, head, theirs, gain_mlp, bias, own_a, other_a, own_b, other_b
        )
        with jax.named_scope(f"partial{layer}"):
            theirs = sent(partial, OVER_TENSOR)
        entry = (middle, partial, theirs)

    keep, give = finish_call(spots, *entry, final_gain.reshape(1, 1024), row_live)
    taken = sent(give, OVER_CORE)
    return jnp.concatenate(
        [jnp.where(s == 0, keep, taken), jnp.where(s == 0, taken, keep)], axis=0
    ).reshape(16, 16, 512)


def solution(mesh):
    in_specs = (
        P("dp", None, None),
        P(),
        P(),
        P("section", "dp", None, "tensor"),
        P("section", "dp", None),
        P("section", "dp", "tensor"),
        P("section", "tensor"),
        P("section", "tensor", "dp"),
        P("section", None),
        P("section", None),
        P(),
    )
    out_specs = P("dp", "section", "tensor")
    return jax.shard_map(local, mesh=mesh, in_specs=in_specs, out_specs=out_specs, check_vma=False)
```
